32 devices in a mesh: dp: 4 (over y, x), space: 8 (over z, core).
Axes of the slice: x: 2, y: 2, z: 4, core: 2. Of those that a mesh axis runs over, the one named last changes fastest.
Arguments:
- fields: bfloat16 [4, 100, 32768], P('dp', None, 'space'), may hold values from -6 to 6
- cell_index: int32 [256, 128], P('space'), may hold values from 0 to 6143
- interp_weight: bfloat16 [256, 16, 128], P('space'), may hold values from 0 to 2, as said below
- w_in: bfloat16 [100, 1024], replicated, may hold values from -0.625 to 0.625
- ln_gain: float32 [1024], replicated, may hold values from 0.5 to 1.5
- w_qkv: bfloat16 [1024, 3072], P('dp'), may hold values from -0.1875 to 0.1875
- w_out: bfloat16 [1024, 1024], P('dp'), may hold values from -3 to 3
Outputs:
- latent: bfloat16 [4, 4096, 1024], P('dp', 'space')
- update: bfloat16 [4, 4096, 1024], P('dp', 'space')
The draws below stay inside these ranges and needn't reach their ends.
Inputs may be any that keep to these rules, and one draw needn't show every extreme that they name: `interp_weight`: in each block the slots from some count on carry zero weight for all its 16 nodes; that count lies between 48 and 128. `cell_index`: indexes a shard's 4096 cells extended by 1024 cells of each neighbouring shard, lower neighbour first.
All inputs are finite; a program needn't handle non-finite values.
Results may differ from the reference program's by a relative error of at most 0.0068.
Values may be sent and summed in bfloat16 or wider, within the bound.
A program may use at most 128 MiB of HBM per device.

```python
import math
import jax
import jax.numpy as jnp
from jax import lax

D = 1024
HEADS = 16
CH = 100
NBLK = 16
SLOTS = 128
NODE_DEV = 512
CELL_DEV = 4096
HEAD_SIZE = 64
HALO_C = 1024
HALO_N = 256
BLK_DEV = 32
SAMPLES = 4
NODES = 4096
CELLS = 32768
BLOCKS = 256
N_SPACE = 8


def draw_interp_weight(key, part):
    count_key, chosen_key, magnitude_key = jax.random.split(key, 3)
    full_shape = (BLOCKS, NBLK, SLOTS)
    live_count = jax.random.randint(count_key, (BLOCKS, 1, 1), 3 * SLOTS // 8, SLOTS + 1)
    slot_index = lax.broadcasted_iota(jnp.int32, full_shape, 2)
    chosen = jax.random.randint(chosen_key, full_shape, 0, 2)
    kept_mask = (slot_index < live_count) & (chosen == 0)
    magnitude = jax.random.uniform(magnitude_key, full_shape, jnp.float32, 0.0, 1.0)
    return jnp.where(kept_mask, magnitude, 0.0).astype(jnp.float32).astype(jnp.bfloat16)


def plant(array, rng, low, largest):
    spot = [jax.random.randint(jax.random.fold_in(rng, axis), (), 0, length) for axis, length in enumerate(array.shape)]
    longest = array.shape.index(max(array.shape))
    beside = spot[:longest] + [(spot[longest] + 1) % array.shape[longest]] + spot[longest + 1:]
    return array.at[tuple(spot)].set(low).at[tuple(beside)].set(largest)


def block_scale(stream_key, dims, shards, least, top_value):
    level, own = 1.0, jax.random.fold_in(stream_key, 6)
    for axis_at, shards_of in shards:
        heights = jnp.exp(jax.random.uniform(jax.random.fold_in(own, axis_at), (shards_of,), jnp.float32, least / len(shards), top_value / len(shards)))
        level = level * jnp.repeat(heights, dims[axis_at] // shards_of).reshape([-1 if axis == axis_at else 1 for axis in range(len(dims))])
    return level


def bell_draw(key, extent, width, bound, shards=(), kind=jnp.bfloat16):
    entries = width * jax.random.normal(key, extent, jnp.float32)
    if shards:
        entries = entries * block_scale(key, extent, shards, -0.22, 0.18)
    return jnp.clip(entries, -bound, bound).astype(kind)


def setup_inputs(seed: int = 0) -> dict:
    seeds = jax.random.split(jax.random.key(seed), 8)
    fields = bell_draw(seeds[0], (SAMPLES, CH, CELLS), 1.0, 6.0, ((0, 4), (2, 8)))
    cell_index = plant(jax.random.randint(seeds[1], (BLOCKS, SLOTS), 0, CELL_DEV + 2 * HALO_C), jax.random.fold_in(seeds[1], 1), 0, (CELL_DEV + 2 * HALO_C) - 1).astype(jnp.int32)
    interp_weight = draw_interp_weight(jax.random.fold_in(seeds[7], 71), 0)
    w_in = bell_draw(seeds[3], (CH, D), CH ** -0.5, 0.625)
    ln_gain = jnp.clip(1.0 + 0.1 * jax.random.normal(seeds[4], (D,), jnp.float32), 0.5, 1.5)
    w_qkv = bell_draw(seeds[5], (D, 3 * D), D ** -0.5, 0.1875, ((0, 4),))
    w_out = bell_draw(seeds[6], (D, D), (max(D // 256, 1)) ** -0.5, 3.0, ((0, 4),))
    return {"fields": fields, "cell_index": cell_index, "interp_weight": interp_weight, "w_in": w_in, "ln_gain": ln_gain, "w_qkv": w_qkv, "w_out": w_out}


def unit_heads(projected):
    head_rows = projected.reshape(projected.shape[0], HEADS, HEAD_SIZE)
    scale_rows = jnp.sqrt(lax.optimization_barrier(jnp.mean(head_rows * head_rows, axis=-1, keepdims=True)) + 1e-06)
    return (head_rows / scale_rows).astype(jnp.bfloat16)

def one_sample(grid_field, cell_index, interp_weight, w_in, ln_gain, w_qkv, w_out):
    owner_shard = jnp.arange(BLOCKS, dtype=jnp.int32) // BLK_DEV
    source = (owner_shard[:, None] * CELL_DEV - HALO_C + cell_index) % CELLS
    picked = jnp.take(grid_field, source.astype(jnp.int32), axis=1).astype(jnp.float32)
    encoded = jnp.einsum('cbs,bns->bnc', picked, interp_weight.astype(jnp.float32))
    encoded = encoded.reshape(NODES, CH).astype(jnp.bfloat16)
    embedded = jnp.dot(encoded, w_in, preferred_element_type=jnp.float32)
    average = lax.optimization_barrier(jnp.mean(embedded, axis=1, keepdims=True))
    centered = embedded - average
    spread = lax.optimization_barrier(jnp.mean(centered * centered, axis=1, keepdims=True))
    normed = (centered / jnp.sqrt(spread + 1e-05) * ln_gain).astype(jnp.bfloat16)
    projected = jnp.dot(normed, w_qkv, preferred_element_type=jnp.float32)
    queries = unit_heads(projected[:, :D])
    keys_all = unit_heads(projected[:, D:2 * D])
    values_all = projected[:, 2 * D:].reshape(NODES, HEADS, HEAD_SIZE).astype(jnp.bfloat16)
    wrapped_keys = jnp.concatenate([keys_all[NODES - HALO_N:], keys_all, keys_all[:HALO_N]], axis=0)
    wrapped_values = jnp.concatenate([values_all[NODES - HALO_N:], values_all, values_all[:HALO_N]], axis=0)

    def attend(shard_index):
        first_row = shard_index * NODE_DEV
        query_rows = lax.dynamic_slice_in_dim(queries, first_row, NODE_DEV, 0).astype(jnp.float32)
        key_rows = lax.dynamic_slice_in_dim(wrapped_keys, first_row, NODE_DEV + 2 * HALO_N, 0).astype(jnp.float32)
        value_rows = lax.dynamic_slice_in_dim(wrapped_values, first_row, NODE_DEV + 2 * HALO_N, 0).astype(jnp.float32)
        scores = jnp.einsum('qhd,khd->hqk', query_rows, key_rows) / math.sqrt(HEAD_SIZE)
        weights = jnp.exp(scores)
        probs = (weights / lax.optimization_barrier(jnp.sum(weights, axis=2, keepdims=True))).astype(jnp.bfloat16)
        mixed_rows = jnp.einsum('hqk,khd->qhd', probs.astype(jnp.float32), value_rows)
        return mixed_rows.astype(jnp.bfloat16).reshape(NODE_DEV, D)
    attended = lax.map(attend, jnp.arange(N_SPACE, dtype=jnp.int32)).reshape(NODES, D)
    update = jnp.dot(attended, w_out, preferred_element_type=jnp.float32).astype(jnp.bfloat16)
    return (embedded.astype(jnp.bfloat16), update)

def reference(fields, cell_index, interp_weight, w_in, ln_gain, w_qkv, w_out):

    def per_sample(grid_field):
        return one_sample(grid_field, cell_index, interp_weight, w_in, ln_gain, w_qkv, w_out)
    latent, update = lax.map(per_sample, fields)
    return (latent, update)
```

```python
import functools

import jax
import jax.numpy as jnp
from jax import lax
from jax.experimental import pallas as pl
from jax.experimental.pallas import tpu as pltpu
from jax.sharding import PartitionSpec as P

HEADS = 16
GROUP_HEADS = 4
F32, BF16 = jnp.float32, jnp.bfloat16
MESH = pl.DeviceIdType.MESH


def kernel(
    n, space, index_ref, field_ref, weight_ref, w_in_ref, gain_ref, w_qkv_ref, w_out_ref,
    latent_ref, update_ref,
    low_ref, high_ref, cells_ref, picked_ref, enc_ref, w_in_full, normed_ref, qkv_ref, out_ref,
    q_ref, k_ref, v_ref, att_ref,
    local_sem, field_send, field_recv, enc_send, enc_recv,
    a_send, a_recv, f_send, f_recv, p_send, p_recv,
):
    d, s = lax.axis_index("dp"), lax.axis_index("space")
    up, down = lax.rem(s + 1, space), lax.rem(s + space - 1, space)
    core = lax.rem(s, 2)
    partner = s + 1 - 2 * core
    channels, cell_count = field_ref.shape
    reach = low_ref.shape[1]
    rows = w_qkv_ref.shape[0]
    half = rows // 2
    quarter = half // 2
    width = w_out_ref.shape[1]
    groups, _, gw3 = qkv_ref.shape
    gw = gw3 // 3
    head_size = gw // GROUP_HEADS
    nodes = latent_ref.shape[0]
    margin = nodes // 2
    window = nodes + 2 * margin
    blocks, per_block, slots = weight_ref.shape
    if n == 4:
        peers = [d + 1 - 2 * lax.rem(d, 2), lax.rem(d + 2, 4), 3 - d]
    else:
        peers = [lax.rem(d + i, n) for i in range(1, n)]

    local = []
    for g in range(groups):
        for t in range(3):
            local.append(pltpu.make_async_copy(
                w_qkv_ref.at[:, pl.ds(t * width + g * gw, gw)],
                qkv_ref.at[g, pl.ds(pl.multiple_of(d * rows, rows), rows), pl.ds(t * gw, gw)],
                local_sem.at[len(local)]))
    local.append(pltpu.make_async_copy(
        w_out_ref, out_ref.at[pl.ds(pl.multiple_of(d * rows, rows), rows), :],
        local_sem.at[len(local)]))
    for copy in local:
        copy.start()

    barrier = pltpu.get_barrier_semaphore()
    for peer in peers:
        pl.semaphore_signal(barrier, inc=1, device_id=(peer, s), device_id_type=MESH)
    for peer in (up, down):
        pl.semaphore_signal(barrier, inc=1, device_id=(d, peer), device_id_type=MESH)
    pl.semaphore_wait(barrier, len(peers) + 2)

    def remote(src, dst, send, recv, device):
        return pltpu.make_async_remote_copy(
            src_ref=src, dst_ref=dst, send_sem=send, recv_sem=recv,
            device_id=device, device_id_type=MESH)

    field_up = remote(field_ref.at[:, pl.ds(cell_count - reach, reach)], low_ref,
                      field_send.at[0], field_recv.at[0], (d, up))
    field_down = remote(field_ref.at[:, pl.ds(0, reach)], high_ref,
                        field_send.at[1], field_recv.at[1], (d, down))
    field_up.start()
    field_down.start()

    def piece(c, slot, lo, size):
        span = pl.ds(pl.multiple_of(slot * rows + lo, size), size)
        return out_ref.at[span, :] if c == groups else qkv_ref.at[c, span, :]

    def own_copy(c, i):
        ref = piece(c, d, core * half, half)
        return remote(ref, ref, a_send.at[c, i], a_recv.at[c, i], (peers[i], s))

    def own_recv(c, i):
        source = peers[i] if n == 4 else peers[n - 2 - i]
        ref = piece(c, source, core * half, half)
        return remote(ref, ref, a_send.at[c, i], a_recv.at[c, i], (peers[i], s)), source

    def swap(c, i, slot, side):
        ref = piece(c, slot, side * half, half)
        return remote(ref, ref, p_send.at[c, i], p_recv.at[c, i], (d, partner))

    direct = 2 if n == 4 else n - 1

    def begin(c):
        mine = local[3 * c:3 * c + 3] if c < groups else local[-1:]
        for copy in mine:
            copy.wait()
        for i in range(direct):
            own_copy(c, i).start()

    def onward(c, i, slot):
        ref = piece(c, slot, core * half + i * quarter, quarter)
        return remote(ref, ref, f_send.at[c, i], f_recv.at[c, i], (peers[1 - i], s))

    def forward(c):
        for i in range(direct):
            copy, source = own_recv(c, i)
            copy.wait_recv()
            if n == 4:
                onward(c, i, source).start()
            swap(c, i, source, core).start()

    def finish(c):
        if n == 4:
            for i in range(2):
                onward(c, i, peers[2]).wait_recv()
            swap(c, 2, peers[2], core).start()
        for i in range(n - 1):
            source = peers[i] if n == 4 else peers[n - 2 - i]
            swap(c, i, source, 1 - core).wait_recv()

    def drain(c):
        for i in range(direct):
            own_copy(c, i).wait_send()
        if n == 4:
            for i in range(2):
                onward(c, i, peers[i]).wait_send()
        for i in range(n - 1):
            source = peers[i] if n == 4 else peers[n - 2 - i]
            swap(c, i, source, core).wait_send()

    begin(0)
    begin(1)

    unit = (lax.broadcasted_iota(jnp.int32, (channels, 128), 0)
            == lax.broadcasted_iota(jnp.int32, (channels, 128), 1)).astype(BF16)

    def turn(source, start, target):
        cells_ref[pl.ds(target, 512), :] = lax.dot_general(
            source[:, pl.ds(start, 512)], unit, (((0,), (0,)), ((), ())),
            preferred_element_type=F32)

    @pl.loop(0, cell_count // 512)
    def _(i):
        turn(field_ref, pl.multiple_of(i * 512, 512), pl.multiple_of(reach + i * 512, 512))

    pad = w_in_full.shape[0]
    w_in_full[pl.ds(pad - 32, 32), :] = jnp.zeros((32, width), BF16)
    w_in_full[pl.ds(0, channels), :] = w_in_ref[...]

    field_up.wait_recv()
    field_down.wait_recv()

    @pl.loop(0, reach // 512)
    def _(i):
        turn(low_ref, pl.multiple_of(i * 512, 512), pl.multiple_of(i * 512, 512))
        turn(high_ref, pl.multiple_of(i * 512, 512),
             pl.multiple_of(reach + cell_count + i * 512, 512))

    def gather(first, last):
        @pl.loop(first, last)
        def _(b):
            base = pl.multiple_of(b * slots, slots)
            for j in range(slots):
                picked_ref[pl.ds(base + j, 1), :] = cells_ref[pl.ds(index_ref[b, j], 1), :]

    gather(0, blocks // 2)
    forward(0)
    begin(2)
    gather(blocks // 2, blocks)

    per_step = 8

    @pl.loop(0, blocks // per_step)
    def _(i):
        for j in range(per_step):
            b = i * per_step + j
            rows_b = picked_ref[pl.ds(pl.multiple_of(b * slots, slots), slots), :].astype(BF16)
            enc_ref[pl.ds(pl.multiple_of(margin + b * per_block, per_block), per_block), :] = jnp.dot(
                weight_ref[b], rows_b, preferred_element_type=F32).astype(BF16)

    enc_up = remote(enc_ref.at[pl.ds(nodes, margin), :], enc_ref.at[pl.ds(0, margin), :],
                    enc_send.at[0], enc_recv.at[0], (d, up))
    enc_down = remote(enc_ref.at[pl.ds(margin, margin), :],
                      enc_ref.at[pl.ds(margin + nodes, margin), :],
                      enc_send.at[1], enc_recv.at[1], (d, down))
    enc_up.start()
    enc_down.start()
    forward(1)
    begin(3)

    def embed(start, own):
        embedded = jnp.dot(enc_ref[pl.ds(start, 128), :], w_in_full[...], preferred_element_type=F32)
        if own:
            latent_ref[pl.ds(start - margin, 128), :] = embedded.astype(BF16)
        average = jnp.mean(embedded, axis=1, keepdims=True)
        centered = embedded - average
        spread = jnp.mean(centered * centered, axis=1, keepdims=True)
        normed_ref[pl.ds(start, 128), :] = (
            centered * lax.rsqrt(spread + 1e-05) * gain_ref[...]).astype(BF16)

    @pl.loop(0, nodes // 128)
    def _(i):
        embed(pl.multiple_of(margin + i * 128, 128), True)

    enc_up.wait_recv()
    enc_down.wait_recv()

    @pl.loop(0, margin // 128)
    def _(i):
        embed(pl.multiple_of(i * 128, 128), False)
        embed(pl.multiple_of(margin + nodes + i * 128, 128), False)

    forward(2)
    begin(4)

    same_head = (lax.broadcasted_iota(jnp.int32, (gw, gw), 0) // head_size
                 == lax.broadcasted_iota(jnp.int32, (gw, gw), 1) // head_size).astype(BF16)
    contract_last = (((1,), (1,)), ((), ()))

    def unit_heads(block, scale):
        squares = block * block
        high = squares.astype(BF16)
        rest = (squares - high.astype(F32)).astype(BF16)
        total = (jnp.dot(high, same_head, preferred_element_type=F32)
                 + jnp.dot(rest, same_head, preferred_element_type=F32))
        return (block * lax.rsqrt(total * (1.0 / head_size) + 1e-06)).astype(BF16) * scale

    def compute(g):
        @pl.loop(0, window // 256)
        def _(i):
            span = pl.ds(pl.multiple_of(i * 256, 256), 256)
            part = jnp.dot(normed_ref[span, :], qkv_ref[g, :, pl.ds(gw, 2 * gw)],
                           preferred_element_type=F32)
            k_ref[span, :] = unit_heads(part[:, :gw], jnp.asarray(1.0, BF16))
            v_ref[span, :] = part[:, gw:].astype(BF16)

        scale = jnp.asarray(head_size ** -0.5, BF16)

        @pl.loop(0, nodes // 256)
        def _(i):
            part = jnp.dot(normed_ref[pl.ds(pl.multiple_of(margin + i * 256, 256), 256), :],
                           qkv_ref[g, :, pl.ds(0, gw)], preferred_element_type=F32)
            q_ref[pl.ds(pl.multiple_of(i * 256, 256), 256), :] = unit_heads(part, scale)

        @pl.loop(0, nodes // 128)
        def _(i):
            span = pl.ds(pl.multiple_of(i * 128, 128), 128)
            queries = q_ref[span, :]
            head_of = lax.broadcasted_iota(jnp.int32, (128, gw), 1) // head_size
            mixed = jnp.zeros((128, gw), F32)
            for h in range(GROUP_HEADS):
                mine = head_of == h
                scores = lax.dot_general(jnp.where(mine, queries, jnp.zeros_like(queries)),
                                         k_ref[...], contract_last, preferred_element_type=F32)
                weights = jnp.exp(scores)
                total = jnp.sum(weights, axis=1, keepdims=True)
                out = jnp.dot(weights.astype(BF16), v_ref[...], preferred_element_type=F32)
                mixed = jnp.where(mine, out * (1.0 / total), mixed)
            att_ref[g, span, :] = mixed.astype(BF16)

    @pl.loop(0, groups)
    def _(g):
        for c in range(groups):
            @pl.when(g == c)
            def _():
                finish(c)
                if c + 3 <= groups:
                    if c + 3 > 2:
                        forward(c + 3)
        compute(g)

    finish(groups)

    @pl.loop(0, nodes // 128)
    def _(i):
        span = pl.ds(pl.multiple_of(i * 128, 128), 128)
        total = jnp.zeros((128, width), F32)
        for g in range(groups):
            total += jnp.dot(att_ref[g, span, :], out_ref[pl.ds(g * gw, gw), :],
                             preferred_element_type=F32)
        update_ref[span, :] = total.astype(BF16)

    for copy in (field_up, field_down, enc_up, enc_down):
        copy.wait_send()
    for c in range(groups + 1):
        drain(c)


def shards(n, space, fields, cell_index, interp_weight, w_in, ln_gain, w_qkv, w_out):
    width = w_out.shape[1]
    blocks, per_block, _ = interp_weight.shape
    nodes = blocks * per_block
    channels, cells = fields.shape[1:]
    reach = cells // 4
    gw = width // HEADS * GROUP_HEADS
    groups = width // gw
    vmem = pl.BlockSpec(memory_space=pltpu.VMEM)
    hbm = pl.BlockSpec(memory_space=pl.ANY)
    dma = pltpu.SemaphoreType.DMA
    latent, update = pl.pallas_call(
        functools.partial(kernel, n, space),
        out_shape=[jax.ShapeDtypeStruct((nodes, width), BF16)] * 2,
        in_specs=[pl.BlockSpec(memory_space=pltpu.SMEM), vmem, vmem, vmem, vmem, hbm, hbm],
        out_specs=[vmem, vmem],
        scratch_shapes=[
            pltpu.VMEM((channels, reach), BF16),
            pltpu.VMEM((channels, reach), BF16),
            pltpu.VMEM((cells + 2 * reach, 128), F32),
            pltpu.VMEM((blocks * 128, 128), F32),
            pltpu.VMEM((2 * nodes, 128), BF16),
            pltpu.VMEM((128, width), BF16),
            pltpu.VMEM((2 * nodes, width), BF16),
            pltpu.VMEM((groups, width, 3 * gw), BF16),
            pltpu.VMEM((width, width), BF16),
            pltpu.VMEM((nodes, gw), BF16),
            pltpu.VMEM((2 * nodes, gw), BF16),
            pltpu.VMEM((2 * nodes, gw), BF16),
            pltpu.VMEM((groups, nodes, gw), BF16),
            dma((3 * groups + 1,)),
            dma((2,)), dma((2,)), dma((2,)), dma((2,)),
            dma((groups + 1, n - 1)), dma((groups + 1, n - 1)),
            dma((groups + 1, 2)), dma((groups + 1, 2)),
            dma((groups + 1, n - 1)), dma((groups + 1, n - 1)),
        ],
        compiler_params=pltpu.CompilerParams(
            collective_id=0, has_side_effects=True, vmem_limit_bytes=60 * 2**20),
    )(cell_index, fields[0], interp_weight, w_in, ln_gain[None], w_qkv, w_out)
    return latent[None], update[None]


def solution(mesh):
    placed = (
        P("dp", None, "space"),
        P("space", None),
        P("space", None, None),
        P(),
        P(),
        P("dp", None),
        P("dp", None),
    )
    return jax.shard_map(
        functools.partial(shards, mesh.shape["dp"], mesh.shape["space"]),
        mesh=mesh,
        in_specs=placed,
        out_specs=(P("dp", "space", None), P("dp", "space", None)),
        check_vma=False,
    )
```

```python
import functools

import jax
import jax.numpy as jnp
from jax import lax
from jax.experimental import pallas as pl
from jax.experimental.pallas import tpu as pltpu
from jax.sharding import PartitionSpec as P

HEADS = 16
GROUP_HEADS = 4
F32, BF16 = jnp.float32, jnp.bfloat16
MESH = pl.DeviceIdType.MESH


def kernel(
    n, space, index_ref, field_ref, weight_ref, w_in_ref, gain_ref, w_qkv_ref, w_out_ref,
    att_out, w_out_full, enc_out,
    low_ref, high_ref, cells_ref, picked_ref, enc_ref, w_in_full, normed_ref, qkv_ref, out_ref,
    q_ref, k_ref, v_ref, att_ref,
    local_sem, leave_sem, field_send, field_recv, enc_send, enc_recv,
    a_send, a_recv, f_send, f_recv, p_send, p_recv,
):
    d, s = lax.axis_index("dp"), lax.axis_index("space")
    up, down = lax.rem(s + 1, space), lax.rem(s + space - 1, space)
    core = lax.rem(s, 2)
    partner = s + 1 - 2 * core
    channels, cell_count = field_ref.shape
    reach = low_ref.shape[1]
    rows = w_qkv_ref.shape[0]
    half = rows // 2
    quarter = half // 2
    width = w_out_ref.shape[1]
    groups, _, gw3 = qkv_ref.shape
    gw = gw3 // 3
    head_size = gw // GROUP_HEADS
    nodes = att_out.shape[0]
    margin = nodes // 2
    window = nodes + 2 * margin
    blocks, per_block, slots = weight_ref.shape
    if n == 4:
        peers = [d + 1 - 2 * lax.rem(d, 2), lax.rem(d + 2, 4), 3 - d]
    else:
        peers = [lax.rem(d + i, n) for i in range(1, n)]

    local = []
    for g in range(groups):
        for t in range(3):
            local.append(pltpu.make_async_copy(
                w_qkv_ref.at[:, pl.ds(t * width + g * gw, gw)],
                qkv_ref.at[g, pl.ds(pl.multiple_of(d * rows, rows), rows), pl.ds(t * gw, gw)],
                local_sem.at[len(local)]))
    local.append(pltpu.make_async_copy(
        w_out_ref, out_ref.at[pl.ds(pl.multiple_of(d * rows, rows), rows), :],
        local_sem.at[len(local)]))
    for copy in local:
        copy.start()

    barrier = pltpu.get_barrier_semaphore()
    for peer in peers:
        pl.semaphore_signal(barrier, inc=1, device_id=(peer, s), device_id_type=MESH)
    for peer in (up, down):
        pl.semaphore_signal(barrier, inc=1, device_id=(d, peer), device_id_type=MESH)
    pl.semaphore_wait(barrier, len(peers) + 2)

    def remote(src, dst, send, recv, device):
        return pltpu.make_async_remote_copy(
            src_ref=src, dst_ref=dst, send_sem=send, recv_sem=recv,
            device_id=device, device_id_type=MESH)

    field_up = remote(field_ref.at[:, pl.ds(cell_count - reach, reach)], low_ref,
                      field_send.at[0], field_recv.at[0], (d, up))
    field_down = remote(field_ref.at[:, pl.ds(0, reach)], high_ref,
                        field_send.at[1], field_recv.at[1], (d, down))
    field_up.start()
    field_down.start()

    def piece(c, slot, lo, size):
        span = pl.ds(pl.multiple_of(slot * rows + lo, size), size)
        return out_ref.at[span, :] if c == groups else qkv_ref.at[c, span, :]

    def own_copy(c, i):
        ref = piece(c, d, core * half, half)
        return remote(ref, ref, a_send.at[c, i], a_recv.at[c, i], (peers[i], s))

    def own_recv(c, i):
        source = peers[i] if n == 4 else peers[n - 2 - i]
        ref = piece(c, source, core * half, half)
        return remote(ref, ref, a_send.at[c, i], a_recv.at[c, i], (peers[i], s)), source

    def swap(c, i, slot, side):
        ref = piece(c, slot, side * half, half)
        return remote(ref, ref, p_send.at[c, i], p_recv.at[c, i], (d, partner))

    direct = 2 if n == 4 else n - 1

    def begin(c):
        mine = local[3 * c:3 * c + 3] if c < groups else local[-1:]
        for copy in mine:
            copy.wait()
        for i in range(direct):
            own_copy(c, i).start()

    def onward(c, i, slot):
        ref = piece(c, slot, core * half + i * quarter, quarter)
        return remote(ref, ref, f_send.at[c, i], f_recv.at[c, i], (peers[1 - i], s))

    def forward(c):
        for i in range(direct):
            copy, source = own_recv(c, i)
            copy.wait_recv()
            if n == 4:
                onward(c, i, source).start()
            swap(c, i, source, core).start()

    def finish(c):
        if n == 4:
            for i in range(2):
                onward(c, i, peers[2]).wait_recv()
            swap(c, 2, peers[2], core).start()
        for i in range(n - 1):
            source = peers[i] if n == 4 else peers[n - 2 - i]
            swap(c, i, source, 1 - core).wait_recv()

    def drain(c):
        for i in range(direct):
            own_copy(c, i).wait_send()
        if n == 4:
            for i in range(2):
                onward(c, i, peers[i]).wait_send()
        for i in range(n - 1):
            source = peers[i] if n == 4 else peers[n - 2 - i]
            swap(c, i, source, core).wait_send()

    begin(0)
    begin(1)
    begin(2)

    unit = (lax.broadcasted_iota(jnp.int32, (channels, 128), 0)
            == lax.broadcasted_iota(jnp.int32, (channels, 128), 1)).astype(BF16)

    def turn(source, start, target):
        cells_ref[pl.ds(target, 512), :] = lax.dot_general(
            source[:, pl.ds(start, 512)], unit, (((0,), (0,)), ((), ())),
            preferred_element_type=F32)

    @pl.loop(0, cell_count // 512, unroll=2)
    def _(i):
        turn(field_ref, pl.multiple_of(i * 512, 512), pl.multiple_of(reach + i * 512, 512))

    pad = w_in_full.shape[0]
    w_in_full[pl.ds(pad - 32, 32), :] = jnp.zeros((32, width), BF16)
    w_in_full[pl.ds(0, channels), :] = w_in_ref[...]

    field_up.wait_recv()
    field_down.wait_recv()

    @pl.loop(0, reach // 512)
    def _(i):
        turn(low_ref, pl.multiple_of(i * 512, 512), pl.multiple_of(i * 512, 512))
        turn(high_ref, pl.multiple_of(i * 512, 512),
             pl.multiple_of(reach + cell_count + i * 512, 512))

    def gather(first, last):
        @pl.loop(first, last)
        def _(b):
            base = pl.multiple_of(b * slots, slots)
            for j in range(slots):
                picked_ref[pl.ds(base + j, 1), :] = cells_ref[pl.ds(index_ref[b, j], 1), :]

    gather(0, blocks // 2)
    forward(0)
    begin(3)
    gather(blocks // 2, blocks)

    per_step = 8

    @pl.loop(0, blocks // per_step)
    def _(i):
        for j in range(per_step):
            b = i * per_step + j
            rows_b = picked_ref[pl.ds(pl.multiple_of(b * slots, slots), slots), :].astype(BF16)
            enc_ref[pl.ds(pl.multiple_of(margin + b * per_block, per_block), per_block), :] = jnp.dot(
                weight_ref[b], rows_b, preferred_element_type=F32).astype(BF16)

    enc_up = remote(enc_ref.at[pl.ds(nodes, margin), :], enc_ref.at[pl.ds(0, margin), :],
                    enc_send.at[0], enc_recv.at[0], (d, up))
    enc_down = remote(enc_ref.at[pl.ds(margin, margin), :],
                      enc_ref.at[pl.ds(margin + nodes, margin), :],
                      enc_send.at[1], enc_recv.at[1], (d, down))
    enc_up.start()
    enc_down.start()
    enc_leave = pltpu.make_async_copy(enc_ref.at[pl.ds(margin, nodes), :], enc_out, leave_sem.at[0])
    enc_leave.start()
    forward(1)
    begin(groups)

    def embed(start):
        embedded = jnp.dot(enc_ref[pl.ds(start, 128), :], w_in_full[...], preferred_element_type=F32)
        average = jnp.mean(embedded, axis=1, keepdims=True)
        centered = embedded - average
        spread = jnp.mean(centered * centered, axis=1, keepdims=True)
        normed_ref[pl.ds(start, 128), :] = (
            centered * lax.rsqrt(spread + 1e-05) * gain_ref[...]).astype(BF16)

    @pl.loop(0, nodes // 128, unroll=2)
    def _(i):
        embed(pl.multiple_of(margin + i * 128, 128))

    enc_up.wait_recv()
    enc_down.wait_recv()

    @pl.loop(0, margin // 128)
    def _(i):
        embed(pl.multiple_of(i * 128, 128))
        embed(pl.multiple_of(margin + nodes + i * 128, 128))

    forward(2)

    same_head = (lax.broadcasted_iota(jnp.int32, (gw, gw), 0) // head_size
                 == lax.broadcasted_iota(jnp.int32, (gw, gw), 1) // head_size).astype(BF16)
    contract_last = (((1,), (1,)), ((), ()))

    def unit_heads(block, scale):
        squares = block * block
        high = squares.astype(BF16)
        rest = (squares - high.astype(F32)).astype(BF16)
        total = (jnp.dot(high, same_head, preferred_element_type=F32)
                 + jnp.dot(rest, same_head, preferred_element_type=F32))
        return (block * lax.rsqrt(total * (1.0 / head_size) + 1e-06)).astype(BF16) * scale

    scale = jnp.asarray(head_size ** -0.5, BF16)
    one = jnp.asarray(1.0, BF16)

    def compute(g):
        for i in range(window // 512):
            span = pl.ds(i * 512, 512)
            part = jnp.dot(normed_ref[span, :], qkv_ref[g, :, pl.ds(gw, 2 * gw)],
                           preferred_element_type=F32)
            k_ref[span, :] = unit_heads(part[:, :gw], one)
            v_ref[span, :] = part[:, gw:].astype(BF16)
        part = jnp.dot(normed_ref[pl.ds(margin, nodes), :], qkv_ref[g, :, pl.ds(0, gw)],
                       preferred_element_type=F32)
        q_ref[...] = unit_heads(part, scale)

        @pl.loop(0, nodes // 128, unroll=2)
        def _(i):
            span = pl.ds(pl.multiple_of(i * 128, 128), 128)
            queries = q_ref[span, :]
            head_of = lax.broadcasted_iota(jnp.int32, (128, gw), 1) // head_size
            stacked = jnp.concatenate(
                [jnp.where(head_of == h, queries, jnp.zeros_like(queries))
                 for h in range(GROUP_HEADS)], axis=0)
            scores = lax.dot_general(stacked, k_ref[...], contract_last,
                                     preferred_element_type=F32)
            weights = jnp.exp(scores)
            total = jnp.sum(weights, axis=1, keepdims=True)
            out = jnp.dot(weights.astype(BF16), v_ref[...], preferred_element_type=F32)
            out = out * (1.0 / total)
            mixed = out[:128]
            for h in range(1, GROUP_HEADS):
                mixed = jnp.where(head_of == h, out[h * 128:(h + 1) * 128], mixed)
            att_ref[g, span, :] = mixed.astype(BF16)

    def leave(g):
        return pltpu.make_async_copy(
            att_ref.at[g], att_out.at[:, pl.ds(g * gw, gw)], leave_sem.at[2 + g])

    w_out_leave = pltpu.make_async_copy(out_ref, w_out_full, leave_sem.at[1])

    @pl.loop(0, groups)
    def _(g):
        for c in range(groups):
            @pl.when(g == c)
            def _():
                finish(c)
                if c + 3 <= groups:
                    forward(c + 3)
                if c:
                    leave(c - 1).start()
                if c == groups - 1:
                    finish(groups)
                    w_out_leave.start()
        compute(g)

    leave(groups - 1).start()
    for g in range(groups):
        leave(g).wait()
    w_out_leave.wait()
    enc_leave.wait()
    for copy in (field_up, field_down, enc_up, enc_down):
        copy.wait_send()
    for c in range(groups + 1):
        drain(c)


def project(enc_ref, w_in_ref, att_ref, w_out_ref, latent_ref, update_ref):
    channels = w_in_ref.shape[0]
    latent_ref[...] = jnp.dot(enc_ref[:, :channels], w_in_ref[...],
                              preferred_element_type=F32).astype(BF16)
    update_ref[...] = jnp.dot(att_ref[...], w_out_ref[...],
                              preferred_element_type=F32).astype(BF16)


def shards(n, space, fields, cell_index, interp_weight, w_in, ln_gain, w_qkv, w_out):
    width = w_out.shape[1]
    blocks, per_block, _ = interp_weight.shape
    nodes = blocks * per_block
    channels, cells = fields.shape[1:]
    reach = cells // 4
    gw = width // HEADS * GROUP_HEADS
    groups = width // gw
    vmem = pl.BlockSpec(memory_space=pltpu.VMEM)
    hbm = pl.BlockSpec(memory_space=pl.ANY)
    dma = pltpu.SemaphoreType.DMA
    attended, w_out_full, encoded = pl.pallas_call(
        functools.partial(kernel, n, space),
        out_shape=[jax.ShapeDtypeStruct(shape, BF16)
                   for shape in ((nodes, width), (width, width), (nodes, 128))],
        in_specs=[pl.BlockSpec(memory_space=pltpu.SMEM), vmem, vmem, vmem, vmem, hbm, hbm],
        out_specs=[hbm, hbm, hbm],
        scratch_shapes=[
            pltpu.VMEM((channels, reach), BF16),
            pltpu.VMEM((channels, reach), BF16),
            pltpu.VMEM((cells + 2 * reach, 128), F32),
            pltpu.VMEM((blocks * 128, 128), F32),
            pltpu.VMEM((2 * nodes, 128), BF16),
            pltpu.VMEM((128, width), BF16),
            pltpu.VMEM((2 * nodes, width), BF16),
            pltpu.VMEM((groups, width, 3 * gw), BF16),
            pltpu.VMEM((width, width), BF16),
            pltpu.VMEM((nodes, gw), BF16),
            pltpu.VMEM((2 * nodes, gw), BF16),
            pltpu.VMEM((2 * nodes, gw), BF16),
            pltpu.VMEM((groups, nodes, gw), BF16),
            dma((3 * groups + 1,)), dma((groups + 2,)),
            dma((2,)), dma((2,)), dma((2,)), dma((2,)),
            dma((groups + 1, n - 1)), dma((groups + 1, n - 1)),
            dma((groups + 1, 2)), dma((groups + 1, 2)),
            dma((groups + 1, n - 1)), dma((groups + 1, n - 1)),
        ],
        compiler_params=pltpu.CompilerParams(
            collective_id=0, has_side_effects=True, vmem_limit_bytes=60 * 2**20),
    )(cell_index, fields[0], interp_weight, w_in, ln_gain[None], w_qkv, w_out)
    step = nodes // 2

    def by_row(size):
        return pl.BlockSpec((step, size), lambda i: (i, 0))

    def whole(array):
        return pl.BlockSpec(array.shape, lambda i: (0, 0))

    latent, update = pl.pallas_call(
        project,
        grid=(nodes // step,),
        out_shape=[jax.ShapeDtypeStruct((nodes, width), BF16)] * 2,
        in_specs=[by_row(128), whole(w_in), by_row(width), whole(w_out_full)],
        out_specs=[by_row(width), by_row(width)],
    )(encoded, w_in, attended, w_out_full)
    return latent[None], update[None]


def solution(mesh):
    placed = (
        P("dp", None, "space"),
        P("space", None),
        P("space", None, None),
        P(),
        P(),
        P("dp", None),
        P("dp", None),
    )
    return jax.shard_map(
        functools.partial(shards, mesh.shape["dp"], mesh.shape["space"]),
        mesh=mesh,
        in_specs=placed,
        out_specs=(P("dp", "space", None), P("dp", "space", None)),
        check_vma=False,
    )
```
